128 devices in a mesh: grp: 4 (over y, x), band: 32 (over z, core).
Axes of the slice: x: 2, y: 2, z: 16, core: 2. Of those that a mesh axis runs over, the one named last changes fastest.
The devices are a block of a 8x8x16 slice.
Arguments:
- source: bfloat16 [1048576, 640], P(('grp', 'band')), parts along dimension 0, may hold values from -96 to 96
- tiles: bfloat16 [8192, 128, 128], P('band'), may hold values from 0 to 0.001953125
- tile_slot: int32 [8192], P('band'), may hold values from 0 to 63, as said below
- tile_dst: int32 [8192], P('band'), may hold values from 0 to 31
- send_index: int32 [32, 64], P('band'), may hold values from 0 to 63
- send_count: int32 [32, 32], P('band'), may hold values from 1 to 2, as said below
- polar_tiles: bfloat16 [2048, 128, 128], P('band'), may hold values from 0 to 0.00024414062
- polar_src: int32 [2048], P('band'), may hold values from 0 to 63
- polar_dst: int32 [2048], P('band'), may hold values from 0 to 31
Outputs:
- model_field: bfloat16 [524288, 640], P(('grp', 'band')), parts along dimension 0
- polar_cap: bfloat16 [16384, 640], P(('grp', 'band')), parts along dimension 0
The draws below stay inside these ranges and needn't reach their ends.
There are 4 independent parts, one for each index of `grp`. The reference program is written for one: setup_inputs(seed, part) draws one part's arguments, and reference() takes and returns one part's arrays. A program takes and returns all parts, laid end to end along the dimension named above; an argument that names none is the same for every part. Nothing has to cross between parts.
Inputs may be any that keep to these rules, and one draw needn't show every extreme that they name: `send_count`: entry [s, o] counts the used slots of band s for owner o; every row has an entry 2, and some owner has 2 from every band. `tile_slot`: tile t names slot s * 2 + j of owner t // 256 with j below send_count[s, t // 256]; every used slot is named by some tile of its owner.
All inputs are finite; a program needn't handle non-finite values.
Results may differ from the reference program's by a relative error of at most 0.001.
Values may be sent and summed in bfloat16 or wider, within the bound.
No kernel may reach another device: no remote copies, remote signals or barrier semaphores. Data moves between devices by JAX's collectives and lax.ppermute only.
A program may use at most 192 MiB of HBM per device.

```python
import jax
import jax.numpy as jnp
from jax import lax

CH = 80
LEV = 8
BLK = 128
CAP = 2
PB_DEV = 1
SB_DEV = 64
TB_DEV = 32
NT_DEV = 256
PT_DEV = 64
OWNERS = 32
SBLOCKS = 2048
NTILES = 8192
PTILES = 2048
PBLOCKS = 32


def shared_counts(key):
    base = jax.random.fold_in(key, 11)
    first, second, third = jax.random.split(base, 3)
    counts = jax.random.randint(first, (OWNERS, OWNERS), 1, CAP + 1)
    column = jax.random.randint(second, (OWNERS,), 0, OWNERS)
    grid = lax.broadcasted_iota(jnp.int32, (OWNERS, OWNERS), 1)
    counts = jnp.where(grid == column[:, None], CAP, counts)
    busiest = jax.random.randint(third, (), 0, OWNERS)
    counts = jnp.where(grid == busiest, CAP, counts)
    return counts.astype(jnp.int32)


def draw_send_count(key, part):
    return shared_counts(key)


def draw_send_index(key, part):
    base = jax.random.fold_in(key, 13)
    return jax.random.randint(base, (OWNERS, OWNERS * CAP), 0, SB_DEV).astype(jnp.int32)


def draw_tile_slot(key, part):
    counts = shared_counts(key)
    base = jax.random.fold_in(key, 17)
    first, second, third = jax.random.split(base, 3)
    position = lax.broadcasted_iota(jnp.int32, (OWNERS, NT_DEV), 1)
    owner = lax.broadcasted_iota(jnp.int32, (OWNERS, NT_DEV), 0)
    random_sender = jax.random.randint(first, (OWNERS, NT_DEV), 0, OWNERS)
    random_pick = jax.random.randint(second, (OWNERS, NT_DEV), 0, CAP * 64)
    cover = position < OWNERS * CAP
    sender = jnp.where(cover, position // CAP, random_sender)
    pick = jnp.where(cover, position % CAP, random_pick)
    pick = pick % counts[sender, owner]
    slots = sender * CAP + pick
    row_keys = jax.random.split(third, OWNERS)
    orders = jax.vmap(lambda k: jax.random.permutation(k, NT_DEV))(row_keys)
    slots = jnp.take_along_axis(slots, orders, axis=1)
    return slots.reshape(OWNERS * NT_DEV).astype(jnp.int32)


def place_ends(entries, rng, least, high):
    spot = [jax.random.randint(jax.random.fold_in(rng, axis), (), 0, length) for axis, length in enumerate(entries.shape)]
    main_axis = entries.shape.index(max(entries.shape))
    next_to = spot[:main_axis] + [(spot[main_axis] + 1) % entries.shape[main_axis]] + spot[main_axis + 1:]
    return entries.at[tuple(spot)].set(least).at[tuple(next_to)].set(high)


def levels(stream_key, dims, pieces, smallest, high):
    level, own = 1.0, jax.random.fold_in(stream_key, 6)
    for axis_at, parts in pieces:
        heights = jnp.exp(jax.random.uniform(jax.random.fold_in(own, axis_at), (parts,), jnp.float32, smallest / len(pieces), high / len(pieces)))
        level = level * jnp.repeat(heights, dims[axis_at] // parts).reshape([-1 if axis == axis_at else 1 for axis in range(len(dims))])
    return level


def gaussian(own_key, shape, spread, most, pieces=(), kind=jnp.bfloat16):
    array = spread * jax.random.normal(own_key, shape, jnp.float32)
    if pieces:
        array = array * levels(own_key, shape, pieces, -0.22, 0.18)
    return jnp.clip(array, -most, most).astype(kind)


def setup_inputs(seed: int = 0, part: int = 0) -> dict:
    splits = jax.random.split(jax.random.key(seed), 10)
    own_keys = jax.random.split(jax.random.fold_in(splits[9], part), 10)
    source = gaussian(own_keys[0], (SBLOCKS * BLK, LEV * CH), 16.0, 96.0, ((0, 32),))
    tiles = jnp.clip(0.001953125 * jax.random.uniform(splits[1], (NTILES, BLK, BLK), jnp.float32) ** levels(splits[1], (NTILES, BLK, BLK), ((0, 32),), -0.2, 0.2), 0.0, 0.001953125).astype(jnp.bfloat16)
    tile_slot = draw_tile_slot(jax.random.fold_in(splits[9], 71), part)
    tile_dst = place_ends(jax.random.randint(splits[3], (NTILES,), 0, TB_DEV), jax.random.fold_in(splits[3], 1), 0, TB_DEV - 1).astype(jnp.int32)
    send_index = draw_send_index(jax.random.fold_in(splits[9], 71), part)
    send_count = draw_send_count(jax.random.fold_in(splits[9], 71), part)
    polar_tiles = jnp.clip(0.00024414062 * jax.random.uniform(splits[6], (PTILES, BLK, BLK), jnp.float32) ** levels(splits[6], (PTILES, BLK, BLK), ((0, 32),), -0.2, 0.2), 0.0, 0.00024414062).astype(jnp.bfloat16)
    polar_src = place_ends(jax.random.randint(splits[7], (PTILES,), 0, SB_DEV), jax.random.fold_in(splits[7], 1), 0, SB_DEV - 1).astype(jnp.int32)
    polar_dst = place_ends(jax.random.randint(splits[8], (PTILES,), 0, PBLOCKS), jax.random.fold_in(splits[8], 1), 0, PBLOCKS - 1).astype(jnp.int32)
    return dict(source=source, tiles=tiles, tile_slot=tile_slot, tile_dst=tile_dst, send_index=send_index, send_count=send_count, polar_tiles=polar_tiles, polar_src=polar_src, polar_dst=polar_dst)


def reference(source, tiles, tile_slot, tile_dst, send_index, send_count, polar_tiles, polar_src, polar_dst):
    feats = LEV * CH
    blocks = source.reshape(OWNERS * SB_DEV, BLK, feats)

    def owner_field(owner):
        start = owner * NT_DEV
        weights = lax.dynamic_slice_in_dim(tiles, start, NT_DEV, 0).astype(jnp.float32)
        slots = lax.dynamic_slice_in_dim(tile_slot, start, NT_DEV, 0)
        places = lax.dynamic_slice_in_dim(tile_dst, start, NT_DEV, 0)
        sender = slots // CAP
        within = slots % CAP
        local = send_index[sender, owner * CAP + within]
        usable = within < send_count[sender, owner]
        inputs = blocks[(sender * SB_DEV + local).astype(jnp.int32)].astype(jnp.float32)
        inputs = jnp.where(usable[:, None, None], inputs, jnp.zeros((), jnp.float32))
        products = jnp.einsum("tps,tsf->tpf", weights, inputs)
        return jax.ops.segment_sum(products, places, num_segments=TB_DEV)

    field = lax.map(owner_field, jnp.arange(OWNERS, dtype=jnp.int32))
    rounded = field.reshape(OWNERS * TB_DEV, BLK, feats).astype(jnp.bfloat16)
    model_field = rounded.reshape(TB_DEV, OWNERS, BLK, feats).transpose(1, 0, 2, 3).reshape(OWNERS * TB_DEV * BLK, feats)

    def band_cap(total, band):
        start = band * PT_DEV
        weights = lax.dynamic_slice_in_dim(polar_tiles, start, PT_DEV, 0).astype(jnp.float32)
        local = lax.dynamic_slice_in_dim(polar_src, start, PT_DEV, 0)
        places = lax.dynamic_slice_in_dim(polar_dst, start, PT_DEV, 0)
        inputs = blocks[(band * SB_DEV + local).astype(jnp.int32)].astype(jnp.float32)
        products = jnp.einsum("tps,tsf->tpf", weights, inputs)
        return total + jax.ops.segment_sum(products, places, num_segments=PB_DEV * OWNERS), None

    cap_sum, _ = lax.scan(band_cap, jnp.zeros((PB_DEV * OWNERS, BLK, feats), jnp.float32), jnp.arange(OWNERS, dtype=jnp.int32))
    polar_cap = cap_sum.reshape(PB_DEV * OWNERS * BLK, feats).astype(jnp.bfloat16)
    return (model_field, polar_cap)
```

```python
import functools

import jax
import jax.numpy as jnp
import numpy as np
from jax import lax
from jax.experimental import pallas as pl
from jax.experimental.pallas import tpu as pltpu
from jax.sharding import PartitionSpec as P


GRP_BAND = ("grp", "band")
CORES = 2
FIRST_PACK = 7
PHASES = (20, 30)
FIRST_SENT = 8
LAST_PLACED = 8
ANY = pl.BlockSpec(memory_space=pl.ANY)
SMEM = pl.BlockSpec(memory_space=pltpu.SMEM)
VMEM = pl.BlockSpec(memory_space=pltpu.VMEM)


def params(mib):
    return pltpu.CompilerParams(vmem_limit_bytes=mib * 2**20)


def cost(flops, moved):
    return pl.CostEstimate(flops=flops, bytes_accessed=moved, transcendentals=0)


def near_to_far(owners):
    chips = owners // CORES
    shifts = [(d, c) for d in range(chips) for c in range(CORES)]
    return sorted(shifts, key=lambda s: (min(s[0], chips - s[0]), s[1], s[0]))


def pairs(owners, shift):
    chips = owners // CORES
    return [
        (i, (i // CORES + shift[0]) % chips * CORES + (i % CORES + shift[1]) % CORES)
        for i in range(owners)
    ]


def moved(owners, me, hop, core):
    chips = owners // CORES
    return lax.rem(me // CORES + hop + chips, chips) * CORES + lax.rem(
        lax.rem(me, CORES) + core, CORES
    )


def pack_kernel(shifts, owners, me_ref, index_ref, count_ref, source_ref, *refs):
    outs, (held, blank, in_sems, out_sems) = refs[: len(shifts)], refs[len(shifts) :]
    per_owner = held.shape[1]
    targets = [moved(owners, me_ref[0], *s) for s in shifts]
    every = [(p, j) for p in range(len(shifts)) for j in range(per_owner)]

    def fetch(p, j):
        block = source_ref.at[index_ref[0, targets[p] * per_owner + j]]
        return pltpu.make_async_copy(block, held.at[p, j], in_sems.at[p, j])

    def put(p, j, block):
        return pltpu.make_async_copy(block, outs[p].at[j], out_sems.at[p, j])

    for p, j in every:
        fetch(p, j).start()
    blank[...] = jnp.zeros_like(blank)
    for p, j in every:
        fetch(p, j).wait()
        used = j < count_ref[0, targets[p]]

        @pl.when(used)
        def _():
            put(p, j, held.at[p, j]).start()

        @pl.when(jnp.logical_not(used))
        def _():
            put(p, j, blank).start()

    for p, j in every:
        put(p, j, held.at[p, j]).wait()


def pack(shifts, owners, me, blocks, index, count):
    inside = blocks.shape[1:]
    per_owner = index.shape[1] // owners
    shape = jax.ShapeDtypeStruct((per_owner, *inside), blocks.dtype)
    size = len(shifts) * per_owner * inside[0] * inside[1] * 2
    return pl.pallas_call(
        functools.partial(pack_kernel, shifts, owners),
        out_shape=[shape] * len(shifts),
        in_specs=[SMEM, SMEM, SMEM, ANY],
        out_specs=[ANY] * len(shifts),
        scratch_shapes=[
            pltpu.VMEM((len(shifts), per_owner, *inside), blocks.dtype),
            pltpu.VMEM(inside, blocks.dtype),
            pltpu.SemaphoreType.DMA((len(shifts), per_owner)),
            pltpu.SemaphoreType.DMA((len(shifts), per_owner)),
        ],
        compiler_params=params(58),
        cost_estimate=cost(0, 2 * size),
        name="pack",
    )(me, index, count, blocks)


def sums_kernel(
    n_inputs, start, bounds_ref, order_ref, slot_ref, place_ref, tiles_ref, *refs
):
    inputs, refs = refs[:n_inputs], refs[n_inputs:]
    if start is None:
        before = None
    else:
        before, refs = refs[0], refs[1:]
    outs, (held, weights, total, in_sems, tile_sems, sum_sem) = refs[:-6], refs[-6:]
    each = inputs[0].shape[0]
    depth = weights.shape[0]
    low, high = bounds_ref[0], bounds_ref[1]

    def fetch(k):
        return pltpu.make_async_copy(inputs[k], held.at[pl.ds(k * each, each)], in_sems.at[k])

    def fetch_tile(i):
        at = lax.rem(i, depth)
        return pltpu.make_async_copy(tiles_ref.at[order_ref[i]], weights.at[at], tile_sems.at[at])

    if before is None:
        for k in range(n_inputs):
            fetch(k).start()
    else:
        for k in range(n_inputs):
            held[pl.ds(k * each, each)] = inputs[k][...]
        sums = pltpu.make_async_copy(before.at[pl.ds(start, total.shape[0])], total, sum_sem)
        sums.start()

    @pl.loop(low, jnp.minimum(low + depth, high))
    def _(i):
        fetch_tile(i).start()

    if before is None:

        @pl.loop(0, total.shape[0])
        def _(b):
            total[b] = jnp.zeros(total.shape[1:], total.dtype)

        for k in range(n_inputs):
            fetch(k).wait()

    else:
        sums.wait()

    @pl.loop(low, high)
    def _(i):
        fetch_tile(i).wait()
        t = order_ref[i]
        place = place_ref[t]
        total[place] += jnp.dot(
            weights[lax.rem(i, depth)], held[slot_ref[t]], preferred_element_type=jnp.float32
        )

        @pl.when(i + depth < high)
        def _():
            fetch_tile(i + depth).start()

    if len(outs) == 1:

        @pl.loop(0, total.shape[0])
        def _(b):
            outs[0][b] = total[b].astype(outs[0].dtype)

    else:
        for b, out in enumerate(outs):
            out[...] = total[b].astype(out.dtype)


def sums(inputs, tiles, bounds, order, slots, places, blocks, start, before, split, dtype):
    each, width, feats = inputs[0].shape
    depth = 16
    if split:
        shape = [jax.ShapeDtypeStruct((width, feats), dtype)] * blocks
    else:
        shape = [jax.ShapeDtypeStruct((blocks, width, feats), dtype)]
    work = tiles.shape[0] * blocks * len(inputs) // 1024
    return pl.pallas_call(
        functools.partial(sums_kernel, len(inputs), None if before is None else start),
        out_shape=shape,
        in_specs=[SMEM] * 4
        + [ANY]
        + ([ANY] * len(inputs) if before is None else [VMEM] * len(inputs) + [ANY]),
        out_specs=[VMEM] * len(shape),
        scratch_shapes=[
            pltpu.VMEM((len(inputs) * each, width, feats), inputs[0].dtype),
            pltpu.VMEM((depth, width, width), tiles.dtype),
            pltpu.VMEM((blocks, width, feats), jnp.float32),
            pltpu.SemaphoreType.DMA((len(inputs),)),
            pltpu.SemaphoreType.DMA((depth,)),
            pltpu.SemaphoreType.DMA,
        ],
        compiler_params=params(58 if before is None else 40),
        cost_estimate=cost(2 * work * width * width * feats, blocks * width * feats * 6),
    )(bounds, order, slots, places, tiles, *inputs, *([] if before is None else [before]))


def place_kernel(shifts, owners, aliased, me_ref, *refs):
    blocks, (out_ref, sems) = refs[aliased : aliased + len(shifts)], refs[-2:]

    def put(p):
        at = moved(owners, me_ref[0], -shifts[p][0], shifts[p][1])
        return pltpu.make_async_copy(blocks[p], out_ref.at[at], sems.at[p])

    for p in range(len(shifts)):
        put(p).start()
    for p in range(len(shifts)):
        put(p).wait()


def place(shifts, owners, me, blocks, out):
    inside = blocks[0].shape
    given = [] if out is None else [out]
    return pl.pallas_call(
        functools.partial(place_kernel, shifts, owners, len(given)),
        out_shape=jax.ShapeDtypeStruct((owners, *inside), blocks[0].dtype),
        in_specs=[SMEM] + [ANY] * len(given) + [VMEM] * len(blocks),
        out_specs=ANY,
        scratch_shapes=[pltpu.SemaphoreType.DMA((len(shifts),))],
        input_output_aliases={1: 0} if given else {},
        compiler_params=params(12),
        cost_estimate=cost(0, 4 * len(blocks) * inside[0] * inside[1]),
        name="place",
    )(me, *given, *blocks)


def looked_up(table, at):
    hit = at[:, None] == lax.broadcasted_iota(jnp.int32, (1, len(table)), 1)
    return jnp.sum(jnp.where(hit, jnp.asarray(table, jnp.int32)[None, :], 0), axis=1)


def apart(owners, here, there):
    chips = owners // CORES
    hop = (there // CORES - here // CORES + chips) % chips
    return hop * CORES + (there % CORES - here % CORES + CORES) % CORES


def grouped(key, groups):
    n = key.shape[0]
    rows = lax.broadcasted_iota(jnp.int32, (n, n), 0)
    cols = lax.broadcasted_iota(jnp.int32, (n, n), 1)
    ahead = (key[None, :] < key[:, None]) | ((key[None, :] == key[:, None]) & (cols < rows))
    rank = jnp.sum(ahead.astype(jnp.int32), axis=1)
    order = jnp.sum(jnp.where(rank[None, :] == rows, cols, 0), axis=1)
    ends = [jnp.zeros((), jnp.int32)] + [
        jnp.sum((key <= g).astype(jnp.int32)) for g in range(groups)
    ]
    return order, [jnp.stack(ends[g : g + 2]) for g in range(groups)]


def polar_kernel(slot_ref, place_ref, tiles_ref, source_ref, out_ref, held, sem):
    copy = pltpu.make_async_copy(source_ref, held, sem)
    copy.start()

    @pl.loop(0, out_ref.shape[0])
    def _(b):
        out_ref[b] = jnp.zeros(out_ref.shape[1:], out_ref.dtype)

    copy.wait()

    @pl.loop(0, tiles_ref.shape[0])
    def _(t):
        out_ref[place_ref[t]] += jnp.dot(
            tiles_ref[t], held[slot_ref[t]], preferred_element_type=jnp.float32
        )


def polar_sums(tiles, slots, places, source, blocks):
    width, feats = source.shape[1:]
    return pl.pallas_call(
        polar_kernel,
        out_shape=jax.ShapeDtypeStruct((blocks, width, feats), jnp.float32),
        in_specs=[SMEM, SMEM, VMEM, ANY],
        out_specs=VMEM,
        scratch_shapes=[pltpu.VMEM(source.shape, source.dtype), pltpu.SemaphoreType.DMA],
        compiler_params=params(58),
        cost_estimate=cost(2 * tiles.size * feats, source.size * 2 + blocks * width * feats * 4),
        name="polar",
    )(slots, places, tiles, source)


def regridded(
    source, tiles, tile_slot, tile_dst, send_index, send_count, polar_tiles, polar_src, polar_dst
):
    owners = lax.axis_size("band")
    width, feats = tiles.shape[1], source.shape[1]
    per_owner = send_index.shape[1] // owners
    blocks = source.reshape(-1, width, feats)
    here = lax.axis_index("band").astype(jnp.int32)
    me = here.reshape(1)

    def send(array, shift):
        return array if shift == (0, 0) else lax.ppermute(array, "band", pairs(owners, shift))

    near = near_to_far(owners)
    own, first, rest = near[:1], near[1:FIRST_PACK], near[FIRST_PACK:]
    arrived = {}
    for part in (first, rest + own):
        packed = pack(part, owners, me, blocks, send_index, send_count)
        for shift, block in zip(part, packed):
            arrived[shift] = send(block, shift)

    cap_part = polar_sums(polar_tiles, polar_src, polar_dst, blocks, owners)
    own_cap = lax.psum_scatter(cap_part, "band", scatter_dimension=0, tiled=True)

    far = near[::-1]
    rows = [s[0] * CORES + s[1] for s in near]
    near_at, far_at = np.argsort(rows), np.argsort(rows[::-1])
    cuts = (0, *PHASES, owners)
    shift_at = looked_up(near_at, apart(owners, tile_slot // per_owner, here))
    places = looked_up(far_at, apart(owners, here, tile_dst))
    phase = sum((shift_at >= c).astype(jnp.int32) for c in PHASES)
    base = looked_up(cuts[:-1], phase)
    slots = (shift_at - base) * per_owner + tile_slot % per_owner
    late = len(PHASES)
    key = phase + ((phase == late) & (places >= FIRST_SENT)).astype(jnp.int32)
    order, bounds = grouped(key, late + 2)
    partial = None
    for p in range(late):
        (partial,) = sums(
            [arrived[s] for s in near[cuts[p] : cuts[p + 1]]],
            tiles, bounds[p], order, slots, places, owners, 0, partial, False, jnp.float32,
        )
    last = [arrived[s] for s in near[cuts[late] :]]
    ready = {}
    for g, (low, high) in enumerate([(0, FIRST_SENT), (FIRST_SENT, owners)]):
        part = sums(
            last, tiles, bounds[late + g], order, slots, places - low, high - low, low, partial,
            True, jnp.bfloat16,
        )
        for shift, block in zip(far[low:high], part):
            ready[shift] = send(block, shift)

    split = owners - LAST_PLACED
    ahead, behind = [far[-1]] + far[:split], far[split:-1]
    placed = place(ahead, owners, me, [ready[s] for s in ahead], None)
    placed = place(behind, owners, me, [ready[s] for s in behind], placed)
    return (placed.reshape(-1, feats), own_cap.reshape(-1, feats).astype(jnp.bfloat16))


def solution(mesh):
    in_specs = (
        P(GRP_BAND, None),
        P("band", None, None),
        P("band"),
        P("band"),
        P("band", None),
        P("band", None),
        P("band", None, None),
        P("band"),
        P("band"),
    )
    out_specs = (P(GRP_BAND, None), P(GRP_BAND, None))
    return jax.shard_map(
        regridded, mesh=mesh, in_specs=in_specs, out_specs=out_specs, check_vma=False
    )
```

```python
import functools

import jax
import jax.numpy as jnp
import numpy as np
from jax import lax
from jax.experimental import pallas as pl
from jax.experimental.pallas import tpu as pltpu
from jax.sharding import PartitionSpec as P


GRP_BAND = ("grp", "band")
CORES = 2
FIRST_PACK = 3
PHASES = (18, 28)
FIRST_SENT = 8
LAST_PLACED = 8
ANY = pl.BlockSpec(memory_space=pl.ANY)
SMEM = pl.BlockSpec(memory_space=pltpu.SMEM)
VMEM = pl.BlockSpec(memory_space=pltpu.VMEM)


def params(mib):
    return pltpu.CompilerParams(vmem_limit_bytes=mib * 2**20)


def cost(flops, moved):
    return pl.CostEstimate(flops=flops, bytes_accessed=moved, transcendentals=0)


def near_to_far(owners):
    chips = owners // CORES
    shifts = [(d, c) for d in range(chips) for c in range(CORES)]
    return sorted(shifts, key=lambda s: (min(s[0], chips - s[0]), s[1], s[0]))


def sending_order(owners):
    near = near_to_far(owners)
    hop = owners // CORES // 2 - 1
    long = [s for s in near if s[0] in (hop, hop + 2) and s[1] == 0]
    return near[:1] + long + [s for s in near[1:] if s not in long]


def pairs(owners, shift):
    chips = owners // CORES
    return [
        (i, (i // CORES + shift[0]) % chips * CORES + (i % CORES + shift[1]) % CORES)
        for i in range(owners)
    ]


def moved(owners, me, hop, core):
    chips = owners // CORES
    return lax.rem(me // CORES + hop + chips, chips) * CORES + lax.rem(
        lax.rem(me, CORES) + core, CORES
    )


def pack_kernel(shifts, owners, me_ref, index_ref, count_ref, source_ref, *refs):
    outs, (held, blank, in_sems, out_sems) = refs[: len(shifts)], refs[len(shifts) :]
    per_owner = held.shape[1]
    targets = [moved(owners, me_ref[0], *s) for s in shifts]
    every = [(p, j) for p in range(len(shifts)) for j in range(per_owner)]

    def fetch(p, j):
        block = source_ref.at[index_ref[0, targets[p] * per_owner + j]]
        return pltpu.make_async_copy(block, held.at[p, j], in_sems.at[p, j])

    def put(p, j, block):
        return pltpu.make_async_copy(block, outs[p].at[j], out_sems.at[p, j])

    for p, j in every:
        fetch(p, j).start()
    blank[...] = jnp.zeros_like(blank)
    for p, j in every:
        fetch(p, j).wait()
        used = j < count_ref[0, targets[p]]

        @pl.when(used)
        def _():
            put(p, j, held.at[p, j]).start()

        @pl.when(jnp.logical_not(used))
        def _():
            put(p, j, blank).start()

    for p, j in every:
        put(p, j, held.at[p, j]).wait()


def pack(shifts, owners, me, blocks, index, count):
    inside = blocks.shape[1:]
    per_owner = index.shape[1] // owners
    shape = jax.ShapeDtypeStruct((per_owner, *inside), blocks.dtype)
    size = len(shifts) * per_owner * inside[0] * inside[1] * 2
    return pl.pallas_call(
        functools.partial(pack_kernel, shifts, owners),
        out_shape=[shape] * len(shifts),
        in_specs=[SMEM, SMEM, SMEM, ANY],
        out_specs=[ANY] * len(shifts),
        scratch_shapes=[
            pltpu.VMEM((len(shifts), per_owner, *inside), blocks.dtype),
            pltpu.VMEM(inside, blocks.dtype),
            pltpu.SemaphoreType.DMA((len(shifts), per_owner)),
            pltpu.SemaphoreType.DMA((len(shifts), per_owner)),
        ],
        compiler_params=params(58),
        cost_estimate=cost(0, 2 * size),
        name="pack",
    )(me, index, count, blocks)


def sums_kernel(
    n_inputs, start, bounds_ref, order_ref, slot_ref, place_ref, tiles_ref, *refs
):
    inputs, refs = refs[:n_inputs], refs[n_inputs:]
    if start is None:
        before = None
    else:
        before, refs = refs[0], refs[1:]
    outs, (held, weights, total, in_sems, tile_sems, sum_sem) = refs[:-6], refs[-6:]
    each = inputs[0].shape[0]
    depth = weights.shape[0]
    low, high = bounds_ref[0], bounds_ref[1]

    def fetch(k):
        return pltpu.make_async_copy(inputs[k], held.at[pl.ds(k * each, each)], in_sems.at[k])

    def fetch_tile(i):
        at = lax.rem(i, depth)
        return pltpu.make_async_copy(tiles_ref.at[order_ref[i]], weights.at[at], tile_sems.at[at])

    if before is None:
        for k in range(n_inputs):
            fetch(k).start()
    else:
        for k in range(n_inputs):
            held[pl.ds(k * each, each)] = inputs[k][...]
        sums = pltpu.make_async_copy(before.at[pl.ds(start, total.shape[0])], total, sum_sem)
        sums.start()

    @pl.loop(low, jnp.minimum(low + depth, high))
    def _(i):
        fetch_tile(i).start()

    if before is None:

        @pl.loop(0, total.shape[0])
        def _(b):
            total[b] = jnp.zeros(total.shape[1:], total.dtype)

        for k in range(n_inputs):
            fetch(k).wait()

    else:
        sums.wait()

    @pl.loop(low, high)
    def _(i):
        fetch_tile(i).wait()
        t = order_ref[i]
        place = place_ref[t]
        total[place] += jnp.dot(
            weights[lax.rem(i, depth)], held[slot_ref[t]], preferred_element_type=jnp.float32
        )

        @pl.when(i + depth < high)
        def _():
            fetch_tile(i + depth).start()

    if len(outs) == 1:

        @pl.loop(0, total.shape[0])
        def _(b):
            outs[0][b] = total[b].astype(outs[0].dtype)

    else:
        for b, out in enumerate(outs):
            out[...] = total[b].astype(out.dtype)


def sums(inputs, tiles, bounds, order, slots, places, blocks, start, before, split, dtype):
    each, width, feats = inputs[0].shape
    depth = 16
    if split:
        shape = [jax.ShapeDtypeStruct((width, feats), dtype)] * blocks
    else:
        shape = [jax.ShapeDtypeStruct((blocks, width, feats), dtype)]
    work = tiles.shape[0] * blocks * len(inputs) // 1024
    return pl.pallas_call(
        functools.partial(sums_kernel, len(inputs), None if before is None else start),
        out_shape=shape,
        in_specs=[SMEM] * 4
        + [ANY]
        + ([ANY] * len(inputs) if before is None else [VMEM] * len(inputs) + [ANY]),
        out_specs=[VMEM] * len(shape),
        scratch_shapes=[
            pltpu.VMEM((len(inputs) * each, width, feats), inputs[0].dtype),
            pltpu.VMEM((depth, width, width), tiles.dtype),
            pltpu.VMEM((blocks, width, feats), jnp.float32),
            pltpu.SemaphoreType.DMA((len(inputs),)),
            pltpu.SemaphoreType.DMA((depth,)),
            pltpu.SemaphoreType.DMA,
        ],
        compiler_params=params(58 if before is None else 40),
        cost_estimate=cost(2 * work * width * width * feats, blocks * width * feats * 6),
    )(bounds, order, slots, places, tiles, *inputs, *([] if before is None else [before]))


def place_kernel(shifts, owners, aliased, me_ref, *refs):
    blocks, (out_ref, sems) = refs[aliased : aliased + len(shifts)], refs[-2:]

    def put(p):
        at = moved(owners, me_ref[0], -shifts[p][0], shifts[p][1])
        return pltpu.make_async_copy(blocks[p], out_ref.at[at], sems.at[p])

    for p in range(len(shifts)):
        put(p).start()
    for p in range(len(shifts)):
        put(p).wait()


def place(shifts, owners, me, blocks, out):
    inside = blocks[0].shape
    given = [] if out is None else [out]
    return pl.pallas_call(
        functools.partial(place_kernel, shifts, owners, len(given)),
        out_shape=jax.ShapeDtypeStruct((owners, *inside), blocks[0].dtype),
        in_specs=[SMEM] + [ANY] * len(given) + [VMEM] * len(blocks),
        out_specs=ANY,
        scratch_shapes=[pltpu.SemaphoreType.DMA((len(shifts),))],
        input_output_aliases={1: 0} if given else {},
        compiler_params=params(12),
        cost_estimate=cost(0, 4 * len(blocks) * inside[0] * inside[1]),
        name="place",
    )(me, *given, *blocks)


def looked_up(table, at):
    hit = at[:, None] == lax.broadcasted_iota(jnp.int32, (1, len(table)), 1)
    return jnp.sum(jnp.where(hit, jnp.asarray(table, jnp.int32)[None, :], 0), axis=1)


def apart(owners, here, there):
    chips = owners // CORES
    hop = (there // CORES - here // CORES + chips) % chips
    return hop * CORES + (there % CORES - here % CORES + CORES) % CORES


def grouped(key, groups):
    n = key.shape[0]
    rows = lax.broadcasted_iota(jnp.int32, (n, n), 0)
    cols = lax.broadcasted_iota(jnp.int32, (n, n), 1)
    ahead = (key[None, :] < key[:, None]) | ((key[None, :] == key[:, None]) & (cols < rows))
    rank = jnp.sum(ahead.astype(jnp.int32), axis=1)
    order = jnp.sum(jnp.where(rank[None, :] == rows, cols, 0), axis=1)
    ends = [jnp.zeros((), jnp.int32)] + [
        jnp.sum((key <= g).astype(jnp.int32)) for g in range(groups)
    ]
    return order, [jnp.stack(ends[g : g + 2]) for g in range(groups)]


def polar_kernel(slot_ref, place_ref, tiles_ref, source_ref, out_ref, held, sem):
    copy = pltpu.make_async_copy(source_ref, held, sem)
    copy.start()

    @pl.loop(0, out_ref.shape[0])
    def _(b):
        out_ref[b] = jnp.zeros(out_ref.shape[1:], out_ref.dtype)

    copy.wait()

    @pl.loop(0, tiles_ref.shape[0])
    def _(t):
        out_ref[place_ref[t]] += jnp.dot(
            tiles_ref[t], held[slot_ref[t]], preferred_element_type=jnp.float32
        )


def polar_sums(tiles, slots, places, source, blocks):
    width, feats = source.shape[1:]
    return pl.pallas_call(
        polar_kernel,
        out_shape=jax.ShapeDtypeStruct((blocks, width, feats), jnp.float32),
        in_specs=[SMEM, SMEM, VMEM, ANY],
        out_specs=VMEM,
        scratch_shapes=[pltpu.VMEM(source.shape, source.dtype), pltpu.SemaphoreType.DMA],
        compiler_params=params(58),
        cost_estimate=cost(2 * tiles.size * feats, source.size * 2 + blocks * width * feats * 4),
        name="polar",
    )(slots, places, tiles, source)


def regridded(
    source, tiles, tile_slot, tile_dst, send_index, send_count, polar_tiles, polar_src, polar_dst
):
    owners = lax.axis_size("band")
    width, feats = tiles.shape[1], source.shape[1]
    per_owner = send_index.shape[1] // owners
    blocks = source.reshape(-1, width, feats)
    here = lax.axis_index("band").astype(jnp.int32)
    me = here.reshape(1)

    def send(array, shift):
        return array if shift == (0, 0) else lax.ppermute(array, "band", pairs(owners, shift))

    near = sending_order(owners)
    own, first, rest = near[:1], near[1:FIRST_PACK], near[FIRST_PACK:]
    arrived = {}
    for part in (first, rest + own):
        packed = pack(part, owners, me, blocks, send_index, send_count)
        for shift, block in zip(part, packed):
            arrived[shift] = send(block, shift)

    cap_part = polar_sums(polar_tiles, polar_src, polar_dst, blocks, owners)
    own_cap = lax.psum_scatter(cap_part, "band", scatter_dimension=0, tiled=True)

    far = near_to_far(owners)[::-1]
    near_at, far_at = (np.argsort([s[0] * CORES + s[1] for s in x]) for x in (near, far))
    cuts = (0, *PHASES, owners)
    shift_at = looked_up(near_at, apart(owners, tile_slot // per_owner, here))
    places = looked_up(far_at, apart(owners, here, tile_dst))
    phase = sum((shift_at >= c).astype(jnp.int32) for c in PHASES)
    base = looked_up(cuts[:-1], phase)
    slots = (shift_at - base) * per_owner + tile_slot % per_owner
    late = len(PHASES)
    key = phase + ((phase == late) & (places >= FIRST_SENT)).astype(jnp.int32)
    order, bounds = grouped(key, late + 2)
    partial = None
    for p in range(late):
        (partial,) = sums(
            [arrived[s] for s in near[cuts[p] : cuts[p + 1]]],
            tiles, bounds[p], order, slots, places, owners, 0, partial, False, jnp.float32,
        )
    last = [arrived[s] for s in near[cuts[late] :]]
    ready = {}
    for g, (low, high) in enumerate([(0, FIRST_SENT), (FIRST_SENT, owners)]):
        part = sums(
            last, tiles, bounds[late + g], order, slots, places - low, high - low, low, partial,
            True, jnp.bfloat16,
        )
        for shift, block in zip(far[low:high], part):
            ready[shift] = send(block, shift)

    split = owners - LAST_PLACED
    ahead, behind = [far[-1]] + far[:split], far[split:-1]
    placed = place(ahead, owners, me, [ready[s] for s in ahead], None)
    placed = place(behind, owners, me, [ready[s] for s in behind], placed)
    return (placed.reshape(-1, feats), own_cap.reshape(-1, feats).astype(jnp.bfloat16))


def solution(mesh):
    in_specs = (
        P(GRP_BAND, None),
        P("band", None, None),
        P("band"),
        P("band"),
        P("band", None),
        P("band", None),
        P("band", None, None),
        P("band"),
        P("band"),
    )
    out_specs = (P(GRP_BAND, None), P(GRP_BAND, None))
    return jax.shard_map(
        regridded, mesh=mesh, in_specs=in_specs, out_specs=out_specs, check_vma=False
    )
```
